32 devices in a mesh: row: 8 (over z, y), col: 4 (over x, core).
Axes of the slice: x: 2, y: 2, z: 4, core: 2. Of those that a mesh axis runs over, the one named last changes fastest.
Arguments:
- tokens: bfloat16 [4096, 4096], P('row', 'col'), may hold values from -6 to 6
- norm_gain: bfloat16 [4096], P('col'), may hold values from 0.099609375 to 1.8984375
- gate_weight: bfloat16 [4096, 10240], P('row', 'col'), may hold values from -0.09375 to 0.09375
- linear_weight: bfloat16 [4096, 10240], P('row', 'col'), may hold values from -0.09375 to 0.09375
- output_weight: bfloat16 [10240, 4096], P('col', 'row'), may hold values from -0.078125 to 0.078125
Outputs:
- block_out: bfloat16 [4096, 4096], P('row', 'col')
The draws below stay inside these ranges and needn't reach their ends.
All inputs are finite; a program needn't handle non-finite values.
Results may differ from the reference program's by a relative error of at most 0.0065.
Values may be sent and summed in bfloat16 or wider, within the bound.
A program may use at most 128 MiB of HBM per device.

```python
import jax
import jax.numpy as jnp
from jax import lax

D = 4096
FF = 10240
TOKENS = 4096


def raised(entries, key, source, target, shards_of, factor):
    owner, partner = [(jnp.arange(entries.shape[dim]) // (entries.shape[dim] // shards_of)).reshape([-1 if axis == dim else 1 for axis in range(entries.ndim)]) for dim in (source, target)]
    chosen = jax.random.permutation(key, shards_of)[partner]
    strong = (owner == chosen) | (owner == (partner + shards_of // 2) % shards_of)
    return jnp.where(strong, factor * entries, entries)


def steps_of(key, dims, pieces, low, high):
    def one(axis_at, shards_of):
        heights = jax.random.uniform(jax.random.fold_in(jax.random.fold_in(key, 6), axis_at), (shards_of,), jnp.float32, low / len(pieces), high / len(pieces))
        return jnp.repeat(jnp.exp(heights), dims[axis_at] // shards_of).reshape((-1,) + (1,) * (len(dims) - axis_at - 1))

    gain = one(*pieces[0])
    for cut in pieces[1:]:
        gain = gain * one(*cut)
    return gain


def scatter_about(key, shape, deviation, reach, pieces=(), dtype=jnp.bfloat16):
    array = deviation * jax.random.normal(key, shape, jnp.float32)
    if pieces:
        array = array * steps_of(key, shape, pieces, -0.22, 0.18)
    return jnp.clip(array, -reach, reach).astype(dtype)


def noise_with(rng, dims, width, bound, pieces, heavy, kind=jnp.bfloat16):
    result = width * jax.random.normal(rng, dims, jnp.float32)
    if pieces:
        result = result * steps_of(rng, dims, pieces, -0.22, 0.18)
    return jnp.clip(raised(result, jax.random.fold_in(rng, 3), *heavy), -bound, bound).astype(kind)


def setup_inputs(seed: int = 0) -> dict:
    key_of = jax.random.split(jax.random.key(seed), 6)
    return {
        "tokens": scatter_about(key_of[0], (TOKENS, D), 1.0, 6.0, ((0, 8), (1, 4))),
        "norm_gain": jnp.clip(1.0 + 0.18 * jax.random.normal(key_of[1], (D,), jnp.float32), 0.099609375, 1.8984375).astype(jnp.bfloat16),
        "gate_weight": scatter_about(key_of[2], (D, FF), D ** -0.5, 0.09375, ((0, 8), (1, 4))),
        "linear_weight": scatter_about(key_of[3], (D, FF), D ** -0.5, 0.09375, ((0, 8), (1, 4))),
        "output_weight": noise_with(key_of[4], (FF, D), FF ** -0.5, 0.078125, ((0, 4), (1, 8)), (0, 1, 8, 2.0)),
    }


def reference(tokens, norm_gain, gate_weight, linear_weight, output_weight):
    values = tokens.astype(jnp.float32)
    meansq = lax.optimization_barrier(jnp.mean(values * values, axis=-1, keepdims=True))
    normed = (values * jax.lax.rsqrt(meansq + 1e-06) * norm_gain.astype(jnp.float32)).astype(jnp.bfloat16)
    gate = jnp.dot(normed, gate_weight, preferred_element_type=jnp.float32)
    linear = jnp.dot(normed, linear_weight, preferred_element_type=jnp.float32)
    hidden = (jax.nn.gelu(gate, approximate=True) * linear).astype(jnp.bfloat16)
    return jnp.dot(hidden, output_weight, preferred_element_type=jnp.float32).astype(jnp.bfloat16)
```

```python
import jax
import jax.numpy as jnp
from jax import lax
from jax.sharding import PartitionSpec as P

LANES = 128
CHUNKS = 2


def gathered(tokens, norm_gain, gate_weight, linear_weight, output_weight):
    whole = lax.all_gather(tokens, "col", axis=1, tiled=True)
    gain_all = lax.all_gather(norm_gain, "col", axis=0, tiled=True)
    normed = rms_normed(whole, gain_all)
    gate = dot(normed, lax.all_gather(gate_weight, "row", axis=0, tiled=True))
    linear = dot(normed, lax.all_gather(linear_weight, "row", axis=0, tiled=True))
    hidden = (jax.nn.gelu(gate, approximate=True) * linear).astype(jnp.bfloat16)
    terms = dot(hidden, lax.all_gather(output_weight, "row", axis=1, tiled=True))
    return lax.psum_scatter(terms, "col", scatter_dimension=1, tiled=True).astype(jnp.bfloat16)


def dot(left, right):
    return jnp.dot(left, right, preferred_element_type=jnp.float32)


def rms_normed(whole, gain_all):
    values = whole.astype(jnp.float32)
    meansq = jnp.mean(values * values, axis=-1, keepdims=True)
    return (values * lax.rsqrt(meansq + 1e-06) * gain_all.astype(jnp.float32)).astype(jnp.bfloat16)


def added(left, right):
    return (left.astype(jnp.float32) + right.astype(jnp.float32)).astype(jnp.bfloat16)


def spread(zs, ys, xs, cores, tokens, norm_gain, gate_weight, linear_weight, output_weight):
    row, col = lax.axis_index("row"), lax.axis_index("col")
    z, y = row // ys, row % ys
    x, core = col // cores, col % cores
    size, width = tokens.shape

    def along_z(value, step, back, ahead):
        pairs = [
            (a * ys + b, (a + step) * ys + b)
            for a in range(zs)
            for b in range(ys)
            if 0 <= a - step * back < zs and 0 <= a + step * ahead < zs
        ]
        return lax.ppermute(value, "row", pairs)

    def round_z(value, step):
        pairs = [(a * ys + b, (a + step) % zs * ys + b) for a in range(zs) for b in range(ys)]
        return lax.ppermute(value, "row", pairs)

    def other_y(value):
        return lax.ppermute(
            value, "row", [(a * ys + b, a * ys + 1 - b) for a in range(zs) for b in range(ys)]
        )

    def other_x(value):
        return lax.ppermute(
            value, "col", [(a * cores + b, (1 - a) * cores + b) for a in range(xs) for b in range(cores)]
        )

    def other_core(value):
        return lax.ppermute(
            value, "col", [(a * cores + b, a * cores + 1 - b) for a in range(xs) for b in range(cores)]
        )

    right, left = [tokens], [tokens]
    for hop in range(zs - 1):
        right.append(along_z(right[-1], 1, hop, 1))
        left.append(along_z(left[-1], -1, hop, 1))
    line = jnp.concatenate(right[:0:-1] + [tokens] + left[1:], axis=0)
    mine = lax.dynamic_slice_in_dim(line, (zs - 1 - z) * size, zs * size, 0)
    across = other_x(mine)
    mine_pair, across_pair = other_core(mine), other_core(across)

    def in_order(flag, first, second):
        return jnp.where(flag == 0, first, second), jnp.where(flag == 0, second, first)

    here = jnp.concatenate(in_order(core, mine, mine_pair), axis=1)
    there = jnp.concatenate(in_order(core, across, across_pair), axis=1)
    whole = jnp.concatenate(in_order(x, here, there), axis=1)
    gain_all = lax.all_gather(norm_gain, "col", axis=0, tiled=True)

    def hidden_part(weight, dim):
        part = weight.shape[dim] // zs
        depth = weight.shape[1 - dim]
        pieces = []
        for step in range(zs):
            piece = lax.dynamic_slice_in_dim(weight, (z + step) % zs * part, part, dim)
            pieces.append((round_z(piece, step) if step else piece, (z - step) % zs))
        out_shape = (part, depth * zs * ys) if dim == 0 else (depth * zs * ys, part)
        result = jnp.zeros(out_shape, weight.dtype)
        for piece, origin in pieces:
            base = origin * ys * depth
            result = lax.dynamic_update_slice_in_dim(result, piece, base + y * depth, 1 - dim)
            result = lax.dynamic_update_slice_in_dim(
                result, other_y(piece), base + (1 - y) * depth, 1 - dim
            )
        return result

    gate_all = hidden_part(gate_weight, 1)
    linear_all = hidden_part(linear_weight, 1)
    output_all = hidden_part(output_weight, 0)

    normed = rms_normed(whole, gain_all)
    gate = dot(normed, gate_all)
    linear = dot(normed, linear_all)
    hidden = (jax.nn.gelu(gate, approximate=True) * linear).astype(jnp.bfloat16)
    hidden = hidden.reshape(zs, size, -1)

    rows = size // CHUNKS
    outs = []
    for chunk in range(CHUNKS):
        left_rows = hidden[:, chunk * rows : (chunk + 1) * rows].reshape(zs * rows, -1)
        terms = dot(left_rows, output_all).astype(jnp.bfloat16)
        terms = terms.reshape(zs * rows, xs, cores, width)
        keep = lax.dynamic_index_in_dim(terms, core, 2, keepdims=False)
        give = lax.dynamic_index_in_dim(terms, 1 - core, 2, keepdims=False)
        terms = added(keep, other_core(give))
        keep = lax.dynamic_index_in_dim(terms, x, 1, keepdims=False)
        give = lax.dynamic_index_in_dim(terms, 1 - x, 1, keepdims=False)
        terms = added(keep, other_x(give))

        def block(at):
            return lax.dynamic_slice_in_dim(terms, jnp.clip(at, 0, zs - 1) * rows, rows, 0)

        total = block(z).astype(jnp.float32)
        for way in (1, -1):
            carried = None
            for far in range(zs - 1, 0, -1):
                send = block(z + way * far)
                if carried is not None:
                    send = added(send, carried)
                carried = along_z(send, way, 0, far)
            total = total + carried.astype(jnp.float32)
        outs.append(total.astype(jnp.bfloat16))
    return jnp.concatenate(outs, axis=0)


def solution(mesh):
    rows, cols = mesh.shape["row"], mesh.shape["col"]

    def local(tokens, norm_gain, gate_weight, linear_weight, output_weight):
        args = (tokens, norm_gain, gate_weight, linear_weight, output_weight)
        zs, ys, xs, cores = rows // 2, 2, cols // 2, 2
        if xs == 2 and gate_weight.shape[1] % (zs * LANES) == 0:
            return spread(zs, ys, xs, cores, *args)
        return gathered(*args)

    return jax.shard_map(
        local,
        mesh=mesh,
        in_specs=(P("row", "col"), P("col"), P("row", "col"), P("row", "col"), P("col", "row")),
        out_specs=P("row", "col"),
        check_vma=False,
    )
```

```python
import jax
import jax.numpy as jnp
from jax import lax
from jax.sharding import PartitionSpec as P


LANES = 128
CHUNKS = 2


def gathered(tokens, norm_gain, gate_weight, linear_weight, output_weight):
    whole = lax.all_gather(tokens, "col", axis=1, tiled=True)
    gain_all = lax.all_gather(norm_gain, "col", axis=0, tiled=True)
    normed = rms_normed(whole, gain_all)
    gate = dot(normed, lax.all_gather(gate_weight, "row", axis=0, tiled=True))
    linear = dot(normed, lax.all_gather(linear_weight, "row", axis=0, tiled=True))
    hidden = (jax.nn.gelu(gate, approximate=True) * linear).astype(jnp.bfloat16)
    terms = dot(hidden, lax.all_gather(output_weight, "row", axis=1, tiled=True))
    return lax.psum_scatter(terms, "col", scatter_dimension=1, tiled=True).astype(jnp.bfloat16)


def dot(left, right):
    return jnp.dot(left, right, preferred_element_type=jnp.float32)


def rms_normed(whole, gain_all):
    values = whole.astype(jnp.float32)
    meansq = jnp.mean(values * values, axis=-1, keepdims=True)
    return (values * lax.rsqrt(meansq + 1e-06) * gain_all.astype(jnp.float32)).astype(jnp.bfloat16)


def added(left, right):
    return (left.astype(jnp.float32) + right.astype(jnp.float32)).astype(jnp.bfloat16)


def spread(zs, ys, xs, cores, tokens, norm_gain, gate_weight, linear_weight, output_weight):
    row, col = lax.axis_index("row"), lax.axis_index("col")
    z, y = row // ys, row % ys
    size, width = tokens.shape
    size_in = gate_weight.shape[0]

    def along_z(value, step, back, ahead):
        pairs = [
            (a * ys + b, (a + step) * ys + b)
            for a in range(zs)
            for b in range(ys)
            if 0 <= a - step * back < zs and 0 <= a + step * ahead < zs
        ]
        return lax.ppermute(value, "row", pairs)

    def round_z(value, step):
        pairs = [(a * ys + b, (a + step) % zs * ys + b) for a in range(zs) for b in range(ys)]
        return lax.ppermute(value, "row", pairs)

    def other_y(value):
        return lax.ppermute(
            value, "row", [(a * ys + b, a * ys + 1 - b) for a in range(zs) for b in range(ys)]
        )

    def other_x(value):
        return lax.ppermute(
            value, "col", [(a * cores + b, (1 - a) * cores + b) for a in range(xs) for b in range(cores)]
        )

    def other_core(value):
        return lax.ppermute(
            value, "col", [(a * cores + b, a * cores + 1 - b) for a in range(xs) for b in range(cores)]
        )

    def to_col(value, other):
        return other(value)

    across = [to_col(tokens, other_x)]
    right, left = [tokens], [tokens]
    for hop in range(zs - 1):
        right.append(along_z(right[-1], 1, hop, 1))
        left.append(along_z(left[-1], -1, hop, 1))
    rest = jnp.concatenate(
        [jnp.where(z >= s, right[s], left[zs - s]) for s in range(1, zs)], axis=0
    )
    across.append(to_col(rest, other_x))
    mine = jnp.concatenate([tokens, rest], axis=0)
    across = jnp.concatenate(across, axis=0)
    mine_pair = to_col(mine, other_core)
    across_pair = to_col(across, other_core)
    whole = jnp.concatenate([mine, mine_pair, across, across_pair], axis=1)
    gains = lax.all_gather(norm_gain, "col", axis=0, tiled=True)
    gain_all = jnp.concatenate(
        [lax.dynamic_slice_in_dim(gains, (col ^ k) * width, width, 0) for k in range(xs * cores)]
    )

    def piece_of(weight, dim, step):
        part = weight.shape[dim] // zs
        return lax.dynamic_slice_in_dim(weight, (z + step) % zs * part, part, dim)

    def both_y(pieces):
        found = []
        for step, piece in enumerate(pieces):
            piece = round_z(piece, step) if step else piece
            passed = other_y(piece)
            found.append(((z - step) % zs * ys + y, piece))
            found.append(((z - step) % zs * ys + 1 - y, passed))
        return found

    depth = size_in
    inputs = both_y(
        [
            jnp.concatenate([piece_of(w, 1, step) for w in (gate_weight, linear_weight)], axis=0)
            for step in range(zs)
        ],
    )
    outputs = both_y([piece_of(output_weight, 0, step) for step in range(zs)])
    part = gate_weight.shape[1] // zs

    gate_all = jnp.zeros((width * xs * cores, part), gate_weight.dtype)
    linear_all, output_all = gate_all, jnp.zeros((part, width * xs * cores), gate_weight.dtype)
    for origin, piece in inputs:
        place = ((origin * depth // width) ^ col) * width + origin * depth % width
        gate_all = lax.dynamic_update_slice_in_dim(gate_all, piece[:depth], place, 0)
        linear_all = lax.dynamic_update_slice_in_dim(linear_all, piece[depth:], place, 0)
    for origin, piece in outputs:
        k = (origin * depth // width) ^ col
        place = ((1 - k % cores) * xs + k // cores) * width + origin * depth % width
        output_all = lax.dynamic_update_slice_in_dim(output_all, piece, place, 1)

    normed = rms_normed(whole, gain_all)
    gate = dot(normed, gate_all)
    linear = dot(normed, linear_all)
    hidden = (jax.nn.gelu(gate, approximate=True) * linear).astype(jnp.bfloat16)
    hidden = hidden.reshape(zs, size, -1)

    rows = size // CHUNKS
    half = xs * width
    outs = []
    for chunk in range(CHUNKS):
        left_rows = hidden[:, chunk * rows : (chunk + 1) * rows].reshape(zs * rows, -1)
        given = dot(left_rows, output_all[:, :half]).astype(jnp.bfloat16)
        came = to_col(given, other_core)
        far_terms = dot(left_rows, output_all[:, half + width :])
        far_terms = added(far_terms, came[:, width:])
        across_terms = to_col(far_terms, other_x)
        terms = dot(left_rows, output_all[:, half : half + width])
        terms = terms + came[:, :width].astype(jnp.float32)
        terms = (terms + across_terms.astype(jnp.float32)).astype(jnp.bfloat16)

        def block(at):
            return lax.dynamic_slice_in_dim(terms, (z - at) % zs * rows, rows, 0)

        total = terms[:rows].astype(jnp.float32)
        for way in (1, -1):
            carried = None
            for far in range(zs - 1, 0, -1):
                send = block(z + way * far)
                if carried is not None:
                    send = added(send, carried)
                carried = along_z(send, way, 0, far)
            total = total + carried.astype(jnp.float32)
        outs.append(total.astype(jnp.bfloat16))
    return jnp.concatenate(outs, axis=0)


def solution(mesh):
    rows, cols = mesh.shape["row"], mesh.shape["col"]
    zs, ys, xs, cores = rows // 2, 2, cols // 2, 2

    def fits(gate_weight):
        return xs == 2 and gate_weight[1] // cols % (zs * LANES) == 0

    def local(tokens, norm_gain, gate_weight, linear_weight, output_weight):
        args = (tokens, norm_gain, gate_weight, linear_weight, output_weight)
        if fits((gate_weight.shape[0], gate_weight.shape[1] * cols)):
            return spread(zs, ys, xs, cores, *args)
        return gathered(*args)

    return jax.shard_map(
        local,
        mesh=mesh,
        in_specs=(P("row", "col"), P("col"), P("row", "col"), P("row", "col"), P("col", "row")),
        out_specs=P("row", "col"),
        check_vma=False,
    )
```

```python
import jax
import jax.numpy as jnp
from jax import lax
from jax.sharding import PartitionSpec as P


LANES = 128
CHUNKS = 2


def gathered(tokens, norm_gain, gate_weight, linear_weight, output_weight):
    whole = lax.all_gather(tokens, "col", axis=1, tiled=True)
    gain_all = lax.all_gather(norm_gain, "col", axis=0, tiled=True)
    normed = rms_normed(whole, gain_all)
    gate = dot(normed, lax.all_gather(gate_weight, "row", axis=0, tiled=True))
    linear = dot(normed, lax.all_gather(linear_weight, "row", axis=0, tiled=True))
    hidden = (jax.nn.gelu(gate, approximate=True) * linear).astype(jnp.bfloat16)
    terms = dot(hidden, lax.all_gather(output_weight, "row", axis=1, tiled=True))
    return lax.psum_scatter(terms, "col", scatter_dimension=1, tiled=True).astype(jnp.bfloat16)


def dot(left, right):
    return jnp.dot(left, right, preferred_element_type=jnp.float32)


def rms_normed(whole, gain_all):
    values = whole.astype(jnp.float32)
    meansq = jnp.mean(values * values, axis=-1, keepdims=True)
    return (values * lax.rsqrt(meansq + 1e-06) * gain_all.astype(jnp.float32)).astype(jnp.bfloat16)


def added(left, right):
    return (left.astype(jnp.float32) + right.astype(jnp.float32)).astype(jnp.bfloat16)


def spread(zs, ys, xs, cores, tokens, norm_gain, gate_weight, linear_weight, output_weight):
    row, col = lax.axis_index("row"), lax.axis_index("col")
    z, y = row // ys, row % ys
    size, width = tokens.shape
    size_in = gate_weight.shape[0]

    def along_z(value, step, back, ahead):
        pairs = [
            (a * ys + b, (a + step) * ys + b)
            for a in range(zs)
            for b in range(ys)
            if 0 <= a - step * back < zs and 0 <= a + step * ahead < zs
        ]
        return lax.ppermute(value, "row", pairs)

    def round_z(value, step):
        pairs = [(a * ys + b, (a + step) % zs * ys + b) for a in range(zs) for b in range(ys)]
        return lax.ppermute(value, "row", pairs)

    def other_y(value):
        return lax.ppermute(
            value, "row", [(a * ys + b, a * ys + 1 - b) for a in range(zs) for b in range(ys)]
        )

    def other_x(value):
        return lax.ppermute(
            value, "col", [(a * cores + b, (1 - a) * cores + b) for a in range(xs) for b in range(cores)]
        )

    def other_core(value):
        return lax.ppermute(
            value, "col", [(a * cores + b, a * cores + 1 - b) for a in range(xs) for b in range(cores)]
        )

    def to_col(value, other):
        return other(value)

    across = [to_col(tokens, other_x)]
    right, left = [tokens], [tokens]
    for hop in range(zs - 1):
        right.append(along_z(right[-1], 1, hop, 1))
        left.append(along_z(left[-1], -1, hop, 1))
    rest = jnp.concatenate(
        [jnp.where(z >= s, right[s], left[zs - s]) for s in range(1, zs)], axis=0
    )
    across.append(to_col(rest, other_x))
    mine = jnp.concatenate([tokens, rest], axis=0)
    across = jnp.concatenate(across, axis=0)
    mine_pair = to_col(mine, other_core)
    across_pair = to_col(across, other_core)
    whole = jnp.concatenate([mine, mine_pair, across, across_pair], axis=1)
    gains = lax.all_gather(norm_gain, "col", axis=0, tiled=True)
    gain_all = jnp.concatenate(
        [lax.dynamic_slice_in_dim(gains, (col ^ k) * width, width, 0) for k in range(xs * cores)]
    )

    def piece_of(weight, dim, step):
        part = weight.shape[dim] // zs
        return lax.dynamic_slice_in_dim(weight, (z + step) % zs * part, part, dim)

    def both_y(pieces):
        found = []
        for step, piece in enumerate(pieces):
            piece = round_z(piece, step) if step else piece
            passed = other_y(piece)
            found.append(((z - step) % zs * ys + y, piece))
            found.append(((z - step) % zs * ys + 1 - y, passed))
        return found

    depth = size_in
    inputs = both_y(
        [
            jnp.concatenate([piece_of(w, 1, step) for w in (gate_weight, linear_weight)], axis=0)
            for step in range(zs)
        ],
    )
    outputs = both_y([piece_of(output_weight, 0, step) for step in range(zs)])

    def joined(found, dim, order, cut=slice(None)):
        steps = []
        for step in range(zs):
            own, passed = found[2 * step][1][cut], found[2 * step + 1][1][cut]
            steps += [jnp.where(y == 0, own, passed), jnp.where(y == 0, passed, own)]
        stack = jnp.concatenate(steps, axis=dim)
        blocks = [
            lax.dynamic_slice_in_dim(stack, (z - (col ^ k)) % zs * width, width, dim) for k in order
        ]
        return jnp.concatenate(blocks, axis=dim)

    near = range(xs * cores)
    gate_all = joined(inputs, 0, near, slice(0, depth))
    linear_all = joined(inputs, 0, near, slice(depth, None))
    output_all = joined(outputs, 1, [k for c in range(cores - 1, -1, -1) for k in near[c::cores]])

    normed = rms_normed(whole, gain_all)
    gate = dot(normed, gate_all)
    linear = dot(normed, linear_all)
    hidden = (jax.nn.gelu(gate, approximate=True) * linear).astype(jnp.bfloat16)
    hidden = hidden.reshape(zs, size, -1)

    rows = size // CHUNKS
    half = xs * width
    outs = []
    for chunk in range(CHUNKS):
        left_rows = hidden[:, chunk * rows : (chunk + 1) * rows].reshape(zs * rows, -1)
        given = dot(left_rows, output_all[:, :half]).astype(jnp.bfloat16)
        came = to_col(given, other_core)
        far_terms = dot(left_rows, output_all[:, half + width :])
        far_terms = added(far_terms, came[:, width:])
        across_terms = to_col(far_terms, other_x)
        terms = dot(left_rows, output_all[:, half : half + width])
        terms = terms + came[:, :width].astype(jnp.float32)
        terms = (terms + across_terms.astype(jnp.float32)).astype(jnp.bfloat16)

        def block(at):
            return lax.dynamic_slice_in_dim(terms, (z - at) % zs * rows, rows, 0)

        total = terms[:rows].astype(jnp.float32)
        for way in (1, -1):
            carried = None
            for far in range(zs - 1, 0, -1):
                send = block(z + way * far)
                if carried is not None:
                    send = added(send, carried)
                carried = along_z(send, way, 0, far)
            total = total + carried.astype(jnp.float32)
        outs.append(total.astype(jnp.bfloat16))
    return jnp.concatenate(outs, axis=0)


def solution(mesh):
    rows, cols = mesh.shape["row"], mesh.shape["col"]
    zs, ys, xs, cores = rows // 2, 2, cols // 2, 2

    def fits(gate_weight):
        return xs == 2 and zs == cols and gate_weight[1] // cols % (zs * LANES) == 0

    def local(tokens, norm_gain, gate_weight, linear_weight, output_weight):
        args = (tokens, norm_gain, gate_weight, linear_weight, output_weight)
        if fits((gate_weight.shape[0], gate_weight.shape[1] * cols)):
            return spread(zs, ys, xs, cores, *args)
        return gathered(*args)

    return jax.shard_map(
        local,
        mesh=mesh,
        in_specs=(P("row", "col"), P("col"), P("row", "col"), P("row", "col"), P("col", "row")),
        out_specs=P("row", "col"),
        check_vma=False,
    )
```
